256 devices in a mesh: row: 64 (over z_hi, y, x, core), col: 4 (over z_lo).
Axes of the slice: x: 4, y: 4, z: 8 (z_hi: 2, z_lo: 4; z = z_hi * 4 + z_lo), core: 2. Of those that a mesh axis runs over, the one named last changes fastest.
Arguments:
- species: float32 [4, 512, 256, 256], P(None, None, 'row', 'col'), may hold values from -6 to 6
- symbol_x: float32 [512], replicated, may hold values from 0.3 to 3
- symbol_y: float32 [256], replicated, may hold values from 0.3 to 3
- symbol_z: float32 [256], replicated, may hold values from 0.3 to 3
Outputs:
- coefficients: float32 [4, 512, 256, 256], P(None, 'row', 'col')
The draws below stay inside these ranges and needn't reach their ends.
All inputs are finite; a program needn't handle non-finite values.
Results may differ from the reference program's by a relative error of at most 0.00007.
Values sent between devices are 32-bit elements; how exact they have to be, the bound alone decides.
A program may use at most 64 MiB of HBM per device.

```python
import jax
import jax.numpy as jnp
from jax import lax

GRID_X = 512
GRID_Y = 256
GRID_Z = 256
FIELDS = 4


def levels(key, extent, split, smallest, largest):
    def one(axis_at, parts):
        draws = jax.random.uniform(jax.random.fold_in(jax.random.fold_in(key, 6), axis_at), (parts,), jnp.float32, smallest / len(split), largest / len(split))
        return jnp.repeat(jnp.exp(draws), extent[axis_at] // parts).reshape((-1,) + (1,) * (len(extent) - axis_at - 1))

    factor_of = one(*split[0])
    for cut in split[1:]:
        factor_of = factor_of * one(*cut)
    return factor_of


def bell_draw(key, shape, width, bound, pieces=(), kind=jnp.bfloat16):
    array = width * jax.random.normal(key, shape, jnp.float32)
    if pieces:
        array = array * levels(key, shape, pieces, -0.22, 0.18)
    return jnp.clip(array, -bound, bound).astype(kind)


def setup_inputs(seed: int = 0) -> dict:
    key_of = jax.random.split(jax.random.key(seed), 5)
    species = bell_draw(key_of[0], (FIELDS, GRID_X, GRID_Y, GRID_Z), 1.0, 6.0, ((2, 64), (3, 4)), jnp.float32)
    symbol_x = jnp.clip(jax.random.uniform(key_of[1], (GRID_X,), jnp.float32, 0.3, 3.0), 0.3, 3.0)
    symbol_y = jnp.clip(jax.random.uniform(key_of[2], (GRID_Y,), jnp.float32, 0.3, 3.0), 0.3, 3.0)
    symbol_z = jnp.clip(jax.random.uniform(key_of[3], (GRID_Z,), jnp.float32, 0.3, 3.0), 0.3, 3.0)
    return dict(species=species, symbol_x=symbol_x, symbol_y=symbol_y, symbol_z=symbol_z)


def transform_table(count):
    rank = jnp.arange(count)
    angle = (jnp.pi / (count + 1)) * (((rank[:, None] + 1) * (rank[None, :] + 1)) % (2 * count + 2)).astype(jnp.float32)
    return jnp.sin(angle) * (2.0 / (count + 1)) ** 0.5


def transform_dim(values, dim):
    moved = jnp.tensordot(values, transform_table(values.shape[dim]), axes=([dim], [0]), precision=lax.Precision.HIGHEST)
    return jnp.moveaxis(moved, -1, dim)


def reference(species, symbol_x, symbol_y, symbol_z):
    coefficients = species
    coefficients = transform_dim(coefficients, 1)
    coefficients = transform_dim(coefficients, 2)
    coefficients = transform_dim(coefficients, 3)
    symbol = symbol_x[:, None, None] + symbol_y[None, :, None] + symbol_z[None, None, :]
    coefficients = coefficients / symbol
    return coefficients
```

```python
import functools

import jax
import jax.numpy as jnp
import ml_dtypes
import numpy as np
from jax import lax
from jax.experimental import pallas as pl
from jax.experimental.pallas import tpu as pltpu
from jax.sharding import PartitionSpec as P

MESH = pl.DeviceIdType.MESH


def transform_table(count):
    rank = np.arange(count)
    step = (rank[:, None] + 1) * (rank[None, :] + 1) % (2 * count + 2)
    table = (np.sin(np.pi / (count + 1) * step) * (2.0 / (count + 1)) ** 0.5).astype(np.float32)
    return table


def halves_of(table):
    high = table.astype(ml_dtypes.bfloat16)
    low = (table - high.astype(np.float32)).astype(ml_dtypes.bfloat16)
    return np.stack([high, low])


def split(values):
    high = values.astype(jnp.bfloat16)
    return high, (values - high.astype(jnp.float32)).astype(jnp.bfloat16)


def product(left, right, dims):
    dot = functools.partial(
        lax.dot_general, dimension_numbers=(dims, ((), ())), preferred_element_type=jnp.float32
    )
    return dot(left[0], right[0]) + (dot(left[0], right[1]) + dot(left[1], right[0]))


def kernel(
    rows, cols,
    field, table_x, table_y, table_z, symbol_x, symbol_y, symbol_z,
    out,
    x_out, y_in, y_out, z_in,
    send_a, recv_a, send_b, recv_b,
):
    fields = field.shape[0]
    row, col = lax.axis_index("row"), lax.axis_index("col")
    share_x = x_out.shape[2]
    share_k = z_in.shape[3]
    pairs = z_in.shape[2]
    lane = lax.broadcasted_iota(jnp.int32, (1, 128), 1)
    low_half = lane < 64

    def join(first, second):
        return (
            jnp.where(low_half, first, pltpu.roll(second, 64, 1)),
            jnp.where(low_half, pltpu.roll(first, 64, 1), second),
        )

    barrier = pltpu.get_barrier_semaphore()

    def greet_row(at, carry):
        pl.semaphore_signal(barrier, inc=1, device_id=(row ^ at, col), device_id_type=MESH)
        return carry

    def greet_col(at, carry):
        pl.semaphore_signal(barrier, inc=1, device_id=(row, col ^ at), device_id_type=MESH)
        return carry

    lax.fori_loop(1, rows, greet_row, 0)
    lax.fori_loop(1, cols, greet_col, 0)

    def stage_x(f, carry):
        modes = product(
            (table_x[0], table_x[1]), split(field[f]), (((1,), (1,)))
        )
        x_out[f] = modes.reshape(x_out.shape[1:])
        y_in[f, row] = x_out[f, row]

        @pl.when(f == 0)
        def _():
            pl.semaphore_wait(barrier, rows + cols - 2)

        def send(at, carry):
            peer = row ^ at
            pltpu.make_async_remote_copy(
                x_out.at[f, peer], y_in.at[f, row], send_a.at[f], recv_a.at[f],
                device_id=(peer, col), device_id_type=MESH,
            ).start()
            return carry

        lax.fori_loop(1, rows, send, 0)
        return carry

    lax.fori_loop(0, fields, stage_x, 0)

    def stage_y(f, carry):
        others = y_in.at[f, pl.ds(0, rows - 1)]
        pltpu.make_async_copy(others, others, recv_a.at[f]).wait()
        columns = []
        for pair in range(pairs):
            even = y_in[f, :, 2 * pair, :]
            odd = y_in[f, :, 2 * pair + 1, :]
            planes = join(even[:, :128], odd[:, :128]) + join(even[:, 128:], odd[:, 128:])
            columns.append(jnp.concatenate(planes, axis=0))
        lines = jnp.concatenate(columns, axis=1)
        modes = product((table_y[0], table_y[1]), split(lines), (((1,), (0,))))
        for pair in range(pairs):
            block = modes[:, 128 * pair : 128 * (pair + 1)].reshape(cols, share_k, 128)
            for at in range(cols):
                y_out[f, at, pair] = block[at]
        z_in[f, col] = y_out[f, col]

        def send(at, carry):
            peer = col ^ at
            pltpu.make_async_remote_copy(
                y_out.at[f, peer], z_in.at[f, col], send_b.at[f], recv_b.at[f],
                device_id=(row, peer), device_id_type=MESH,
            ).start()
            return carry

        lax.fori_loop(1, cols, send, 0)
        return carry

    lax.fori_loop(0, fields, stage_y, 0)

    here = lax.broadcasted_iota(jnp.int32, (share_k, 256), 0) + col * share_k
    there = lax.broadcasted_iota(jnp.int32, (share_k, 256), 1)
    part_y = jnp.sum(jnp.where(here == there, symbol_y[...], 0.0), axis=1, keepdims=True)
    symbol_yz = part_y + symbol_z[...]

    def stage_z(f, carry):
        others = z_in.at[f, pl.ds(0, cols - 1)]
        pltpu.make_async_copy(others, others, recv_b.at[f]).wait()
        lines = []
        for pair in range(pairs):
            even0, odd0 = join(z_in[f, 0, pair], z_in[f, 1, pair])
            even1, odd1 = join(z_in[f, 2, pair], z_in[f, 3, pair])
            lines.append(jnp.concatenate([even0, even1], axis=1))
            lines.append(jnp.concatenate([odd0, odd1], axis=1))
        lines = jnp.concatenate(lines, axis=0)
        modes = product(split(lines), (table_z[0], table_z[1]), (((1,), (0,))))
        for x in range(share_x):
            symbol = symbol_yz + symbol_x[row * share_x + x]
            out[f, x] = modes[share_k * x : share_k * (x + 1)] / symbol
        return carry

    lax.fori_loop(0, fields, stage_z, 0)

    def drain(f, carry):
        sent = x_out.at[f, pl.ds(0, rows - 1)]
        pltpu.make_async_copy(sent, sent, send_a.at[f]).wait()
        sent = y_out.at[f, pl.ds(0, cols - 1)]
        pltpu.make_async_copy(sent, sent, send_b.at[f]).wait()
        return carry

    lax.fori_loop(0, fields, drain, 0)


def on_device(rows, cols, tables, species, symbol_x, symbol_y, symbol_z):
    fields, grid_x, share_y, share_z = species.shape
    grid_y, grid_z = share_y * rows, share_z * cols
    share_x, share_k = grid_x // rows, grid_y // cols
    field = species.transpose(0, 2, 3, 1).reshape(fields, share_y * share_z, grid_x)
    vmem = pl.BlockSpec(memory_space=pltpu.VMEM)
    smem = pl.BlockSpec(memory_space=pltpu.SMEM)
    return pl.pallas_call(
        functools.partial(kernel, rows, cols),
        out_shape=jax.ShapeDtypeStruct((fields, share_x, share_k, grid_z), jnp.float32),
        in_specs=[vmem, vmem, vmem, vmem, smem, vmem, vmem],
        out_specs=vmem,
        scratch_shapes=[
            pltpu.VMEM((fields, rows, share_x, share_y * share_z), jnp.float32),
            pltpu.VMEM((fields, rows, share_x, share_y * share_z), jnp.float32),
            pltpu.VMEM((fields, cols, share_x // 2, share_k, 2 * share_z), jnp.float32),
            pltpu.VMEM((fields, cols, share_x // 2, share_k, 2 * share_z), jnp.float32),
            pltpu.SemaphoreType.DMA((fields,)),
            pltpu.SemaphoreType.DMA((fields,)),
            pltpu.SemaphoreType.DMA((fields,)),
            pltpu.SemaphoreType.DMA((fields,)),
        ],
        compiler_params=pltpu.CompilerParams(
            collective_id=0, has_side_effects=True, vmem_limit_bytes=60 * 2**20
        ),
    )(field, *tables, symbol_x, symbol_y[None], symbol_z[None])


def solution(mesh):
    rows, cols = mesh.shape["row"], mesh.shape["col"]

    def whole(species, symbol_x, symbol_y, symbol_z):
        _, grid_x, grid_y, grid_z = species.shape
        share_y = grid_y // rows
        order = np.arange(grid_y).reshape(rows, share_y).T.reshape(-1)
        tables = (
            jnp.asarray(halves_of(transform_table(grid_x))),
            jnp.asarray(halves_of(transform_table(grid_y)[:, order])),
            jnp.asarray(halves_of(transform_table(grid_z))),
        )
        return jax.shard_map(
            functools.partial(on_device, rows, cols),
            mesh=mesh,
            in_specs=((P(), P(), P()), P(None, None, "row", "col"), P(), P(), P()),
            out_specs=P(None, "row", "col", None),
            check_vma=False,
        )(tables, species, symbol_x, symbol_y, symbol_z)

    return whole
```

```python
import functools

import jax
import jax.numpy as jnp
import ml_dtypes
import numpy as np
from jax import lax
from jax.experimental import pallas as pl
from jax.experimental.pallas import tpu as pltpu
from jax.sharding import PartitionSpec as P

MESH = pl.DeviceIdType.MESH


def transform_table(count):
    rank = np.arange(count)
    step = (rank[:, None] + 1) * (rank[None, :] + 1) % (2 * count + 2)
    table = (np.sin(np.pi / (count + 1) * step) * (2.0 / (count + 1)) ** 0.5).astype(np.float32)
    return table


def halves_of(table):
    high = table.astype(ml_dtypes.bfloat16)
    low = (table - high.astype(np.float32)).astype(ml_dtypes.bfloat16)
    return np.stack([high, low])


def split(values):
    high = values.astype(jnp.bfloat16)
    return high, (values - high.astype(jnp.float32)).astype(jnp.bfloat16)


def product(left, right, dims):
    dot = functools.partial(
        lax.dot_general, dimension_numbers=(dims, ((), ())), preferred_element_type=jnp.float32
    )
    return dot(left[0], right[0]) + (dot(left[0], right[1]) + dot(left[1], right[0]))


def kernel(
    rows, cols,
    field_hbm, table_x_hbm, table_y_hbm, table_z_hbm, symbol_x_hbm, symbol_y_hbm, symbol_z_hbm,
    out,
    field, table_x, table_y, table_z, symbol_x, symbol_y, symbol_z,
    x_out, middle, y_in, y_out, z_in,
    send_m, recv_m, send_a, recv_a, send_b, recv_b, load_field, load_rest,
):
    fields = field.shape[0]
    row, col = lax.axis_index("row"), lax.axis_index("col")
    share_x = x_out.shape[2]
    share_k = z_in.shape[3]
    pairs = z_in.shape[2]

    barrier = pltpu.get_barrier_semaphore()

    half = rows // 2
    partner = row ^ half
    plane = row // half * half
    place = row - plane

    def greet_row(at, carry):
        pl.semaphore_signal(barrier, inc=1, device_id=(row ^ at, col), device_id_type=MESH)
        return carry

    def greet_col(at, carry):
        pl.semaphore_signal(barrier, inc=1, device_id=(row, col ^ at), device_id_type=MESH)
        return carry

    loads = [pltpu.make_async_copy(field_hbm.at[f], field.at[f], load_field.at[f]) for f in range(fields)]
    rest = [
        pltpu.make_async_copy(source, target, load_rest.at[at])
        for at, (source, target) in enumerate((
            (table_x_hbm, table_x), (table_y_hbm, table_y), (table_z_hbm, table_z),
            (symbol_x_hbm, symbol_x), (symbol_y_hbm, symbol_y), (symbol_z_hbm, symbol_z),
        ))
    ]
    loads[0].start()
    rest[0].start()
    pl.semaphore_signal(barrier, inc=1, device_id=(partner, col), device_id_type=MESH)
    lax.fori_loop(1, half, greet_row, 0)
    lax.fori_loop(1, cols, greet_col, 0)
    for copy in loads[1:] + rest[1:]:
        copy.start()
    rest[0].wait()

    lane = lax.broadcasted_iota(jnp.int32, (1, 128), 1)
    low_half = lane < 64

    def join(first, second):
        return (
            jnp.where(low_half, first, pltpu.roll(second, 64, 1)),
            jnp.where(low_half, pltpu.roll(first, 64, 1), second),
        )

    def compute_x(f):
        pltpu.make_async_copy(field_hbm.at[f], field.at[f], load_field.at[f]).wait()
        modes = product((table_x[0], table_x[1]), split(field[f]), (((1,), (1,))))
        x_out[f] = modes.reshape(x_out.shape[1:])
        y_in[f, row] = x_out[f, row]

    def send_x(f):
        pltpu.make_async_remote_copy(
            x_out.at[f, pl.ds(half - plane, half)], middle.at[f], send_m.at[f], recv_m.at[f],
            device_id=(partner, col), device_id_type=MESH,
        ).start()

        def send(at, carry):
            peer = row ^ at
            pltpu.make_async_remote_copy(
                x_out.at[f, peer], y_in.at[f, row], send_a.at[f], recv_a.at[f],
                device_id=(peer, col), device_id_type=MESH,
            ).start()
            return carry

        lax.fori_loop(1, half, send, 0)

    def pass_on(f):
        pltpu.make_async_copy(middle.at[f], middle.at[f], recv_m.at[f]).wait()

        def send(at, carry):
            peer = row ^ at
            pltpu.make_async_remote_copy(
                middle.at[f, place ^ at], y_in.at[f, partner], send_a.at[f], recv_a.at[f],
                device_id=(peer, col), device_id_type=MESH,
            ).start()
            return carry

        lax.fori_loop(1, half, send, 0)
        y_in[f, partner] = middle[f, place]

    def stage_y(f):
        others = y_in.at[f, pl.ds(0, rows - 2)]
        pltpu.make_async_copy(others, others, recv_a.at[f]).wait()
        columns = []
        for pair in range(pairs):
            even = y_in[f, :, 2 * pair, :]
            odd = y_in[f, :, 2 * pair + 1, :]
            planes = join(even[:, :128], odd[:, :128]) + join(even[:, 128:], odd[:, 128:])
            columns.append(jnp.concatenate(planes, axis=0))
        lines = jnp.concatenate(columns, axis=1)
        modes = product((table_y[0], table_y[1]), split(lines), (((1,), (0,))))
        for pair in range(pairs):
            block = modes[:, 128 * pair : 128 * (pair + 1)].reshape(cols, share_k, 128)
            for at in range(cols):
                y_out[f, at, pair] = block[at]
        z_in[f, col] = y_out[f, col]

        def send(at, carry):
            peer = col ^ at
            pltpu.make_async_remote_copy(
                y_out.at[f, peer], z_in.at[f, col], send_b.at[f], recv_b.at[f],
                device_id=(row, peer), device_id_type=MESH,
            ).start()
            return carry

        lax.fori_loop(1, cols, send, 0)

    def first(f, carry):
        compute_x(f)

        @pl.when(f == 0)
        def _():
            pl.semaphore_wait(barrier, half + cols - 1)

        send_x(f)
        return carry

    lax.fori_loop(0, fields, first, 0)
    for copy in rest[1:]:
        copy.wait()

    def second(f, carry):
        pass_on(f)
        stage_y(f)
        return carry

    lax.fori_loop(0, fields, second, 0)

    here = lax.broadcasted_iota(jnp.int32, (share_k, 256), 0) + col * share_k
    there = lax.broadcasted_iota(jnp.int32, (share_k, 256), 1)
    part_y = jnp.sum(jnp.where(here == there, symbol_y[...], 0.0), axis=1, keepdims=True)
    symbol_yz = part_y + symbol_z[...]
    at_x = lax.broadcasted_iota(jnp.int32, symbol_x.shape, 1) - row * share_x

    def stage_z(f, carry):
        others = z_in.at[f, pl.ds(0, cols - 1)]
        pltpu.make_async_copy(others, others, recv_b.at[f]).wait()
        lines = []
        for pair in range(pairs):
            even0, odd0 = join(z_in[f, 0, pair], z_in[f, 1, pair])
            even1, odd1 = join(z_in[f, 2, pair], z_in[f, 3, pair])
            lines.append(jnp.concatenate([even0, even1], axis=1))
            lines.append(jnp.concatenate([odd0, odd1], axis=1))
        lines = jnp.concatenate(lines, axis=0)
        modes = product(split(lines), (table_z[0], table_z[1]), (((1,), (0,))))
        for x in range(share_x):
            part_x = jnp.sum(jnp.where(at_x == x, symbol_x[...], 0.0), axis=1, keepdims=True)
            out[f, x] = modes[share_k * x : share_k * (x + 1)] / (part_x + symbol_yz)
        return carry

    lax.fori_loop(0, fields, stage_z, 0)

    def drain(f, carry):
        pltpu.make_async_copy(middle.at[f], middle.at[f], send_m.at[f]).wait()
        sent = x_out.at[f, pl.ds(0, rows - 2)]
        pltpu.make_async_copy(sent, sent, send_a.at[f]).wait()
        sent = y_out.at[f, pl.ds(0, cols - 1)]
        pltpu.make_async_copy(sent, sent, send_b.at[f]).wait()
        return carry

    lax.fori_loop(0, fields, drain, 0)


def on_device(rows, cols, tables, species, symbol_x, symbol_y, symbol_z):
    fields, grid_x, share_y, share_z = species.shape
    grid_y, grid_z = share_y * rows, share_z * cols
    share_x, share_k = grid_x // rows, grid_y // cols
    field = species.transpose(0, 2, 3, 1).reshape(fields, share_y * share_z, grid_x)
    hbm = pl.BlockSpec(memory_space=pltpu.HBM)
    return pl.pallas_call(
        functools.partial(kernel, rows, cols),
        out_shape=pltpu.VMEM((fields, share_x, share_k, grid_z), jnp.float32),
        in_specs=[hbm] * 7,
        out_specs=pl.BlockSpec(memory_space=pltpu.VMEM),
        scratch_shapes=[
            pltpu.VMEM(field.shape, jnp.float32),
            *(pltpu.VMEM(table.shape, table.dtype) for table in tables),
            pltpu.VMEM((1, grid_x), jnp.float32),
            pltpu.VMEM((1, grid_y), jnp.float32),
            pltpu.VMEM((1, grid_z), jnp.float32),
            pltpu.VMEM((fields, rows, share_x, share_y * share_z), jnp.float32),
            pltpu.VMEM((fields, rows // 2, share_x, share_y * share_z), jnp.float32),
            pltpu.VMEM((fields, rows, share_x, share_y * share_z), jnp.float32),
            pltpu.VMEM((fields, cols, share_x // 2, share_k, 2 * share_z), jnp.float32),
            pltpu.VMEM((fields, cols, share_x // 2, share_k, 2 * share_z), jnp.float32),
            pltpu.SemaphoreType.DMA((fields,)),
            pltpu.SemaphoreType.DMA((fields,)),
            pltpu.SemaphoreType.DMA((fields,)),
            pltpu.SemaphoreType.DMA((fields,)),
            pltpu.SemaphoreType.DMA((fields,)),
            pltpu.SemaphoreType.DMA((fields,)),
            pltpu.SemaphoreType.DMA((fields,)),
            pltpu.SemaphoreType.DMA((6,)),
        ],
        compiler_params=pltpu.CompilerParams(
            collective_id=0, has_side_effects=True, vmem_limit_bytes=20 * 2**20
        ),
    )(*(pltpu.with_memory_space_constraint(a, pltpu.HBM) for a in (field, *tables, symbol_x[None], symbol_y[None], symbol_z[None])))


def solution(mesh):
    rows, cols = mesh.shape["row"], mesh.shape["col"]

    def whole(species, symbol_x, symbol_y, symbol_z):
        _, grid_x, grid_y, grid_z = species.shape
        share_y = grid_y // rows
        order = np.arange(grid_y).reshape(rows, share_y).T.reshape(-1)
        tables = (
            jnp.asarray(halves_of(transform_table(grid_x))),
            jnp.asarray(halves_of(transform_table(grid_y)[:, order])),
            jnp.asarray(halves_of(transform_table(grid_z))),
        )
        return jax.shard_map(
            functools.partial(on_device, rows, cols),
            mesh=mesh,
            in_specs=((P(), P(), P()), P(None, None, "row", "col"), P(), P(), P()),
            out_specs=P(None, "row", "col", None),
            check_vma=False,
        )(tables, species, symbol_x, symbol_y, symbol_z)

    return whole
```

```python
import functools
import math

import jax
import jax.numpy as jnp
import ml_dtypes
import numpy as np
from jax import lax
from jax.experimental import pallas as pl
from jax.experimental.pallas import tpu as pltpu
from jax.sharding import PartitionSpec as P

MESH = pl.DeviceIdType.MESH


def transform_table(count):
    rank = np.arange(count)
    step = (rank[:, None] + 1) * (rank[None, :] + 1) % (2 * count + 2)
    table = (np.sin(np.pi / (count + 1) * step) * (2.0 / (count + 1)) ** 0.5).astype(np.float32)
    return table


def halves_of(table):
    high = table.astype(ml_dtypes.bfloat16)
    low = (table - high.astype(np.float32)).astype(ml_dtypes.bfloat16)
    return np.stack([high, low])


def split(values):
    high = values.astype(jnp.bfloat16)
    return high, (values - high.astype(jnp.float32)).astype(jnp.bfloat16)


def product(left, right, dims):
    dot = functools.partial(
        lax.dot_general, dimension_numbers=(dims, ((), ())), preferred_element_type=jnp.float32
    )
    return dot(left[0], right[0]) + (dot(left[0], right[1]) + dot(left[1], right[0]))


def kernel(
    rows, cols,
    field_hbm, table_x_hbm, table_y_hbm, table_z_hbm, symbol_x_hbm, symbol_y_hbm, symbol_z_hbm,
    out,
    field, table_x, table_y, table_z, symbol_x, symbol_y, symbol_z,
    x_out, relay, middle, y_in, y_out, z_in,
    token, send_r, recv_r, send_w, send_m, recv_m, send_a, recv_a, send_b, recv_b, load_field, load_rest,
):
    fields = field.shape[0]
    row, col = lax.axis_index("row"), lax.axis_index("col")
    share_x = x_out.shape[2]
    share_k = z_in.shape[3]
    pairs = z_in.shape[2]

    barrier = pltpu.get_barrier_semaphore()

    half = rows // 2
    partner = row ^ half
    plane = row // half * half
    place = row - plane
    side = math.isqrt(half // 2)
    layers = 2 * cols
    layer = row // half * cols + col
    at_x, at_y = lax.rem(place // 2, side), place // (2 * side)

    def ring(step):
        there = lax.rem(layer + step + layers, layers)
        return place + there // cols * half, lax.rem(there, cols)

    def beside_x(step):
        return row + 2 * (lax.rem(at_x + step + side, side) - at_x), col

    def beside_y(step):
        return row + 2 * side * (lax.rem(at_y + step + side, side) - at_y), col

    def signal(semaphore, *devices):
        for device in devices:
            pl.semaphore_signal(semaphore, inc=1, device_id=device, device_id_type=MESH)

    loads = [pltpu.make_async_copy(field_hbm.at[f], field.at[f], load_field.at[f]) for f in range(fields)]
    rest = [
        pltpu.make_async_copy(source, target, load_rest.at[at])
        for at, (source, target) in enumerate((
            (table_x_hbm, table_x), (table_y_hbm, table_y), (table_z_hbm, table_z),
            (symbol_x_hbm, symbol_x), (symbol_y_hbm, symbol_y), (symbol_z_hbm, symbol_z),
        ))
    ]
    straight, relayed = range(fields // 2), range(fields // 2, fields)
    loads[relayed[0]].start()
    rest[0].start()
    signal(
        barrier, ring(1), ring(-1), (row ^ 1, col),
        beside_x(1), beside_x(-1), beside_y(1), beside_y(-1),
    )
    for f in (*relayed[1:], *straight):
        loads[f].start()
    for copy in rest[1:]:
        copy.start()
    rest[0].wait()

    lane = lax.broadcasted_iota(jnp.int32, (1, 128), 1)
    low_half = lane < 64

    def join(first, second):
        return (
            jnp.where(low_half, first, pltpu.roll(second, 64, 1)),
            jnp.where(low_half, pltpu.roll(first, 64, 1), second),
        )

    def compute_x(f):
        pltpu.make_async_copy(field_hbm.at[f], field.at[f], load_field.at[f]).wait()
        modes = product((table_x[0], table_x[1]), split(field[f]), (((1,), (1,))))
        x_out[f] = modes.reshape(x_out.shape[1:])
        y_in[f, row] = x_out[f, row]

    def relay_of(f, way):
        return pltpu.make_async_remote_copy(
            x_out.at[f, pl.ds(half - plane + way * (half // 2), half // 2)],
            relay.at[f - relayed[0], way], send_r.at[f - relayed[0], way], recv_r.at[f - relayed[0], way],
            device_id=ring(1 - 2 * way), device_id_type=MESH,
        )

    def forward_of(f, way):
        return pltpu.make_async_remote_copy(
            relay.at[f - relayed[0], way], middle.at[f, pl.ds(way * (half // 2), half // 2)],
            send_w.at[f - relayed[0], way], recv_m.at[f],
            device_id=ring(3 - 6 * way), device_id_type=MESH,
        )

    def across(f):
        return pltpu.make_async_remote_copy(
            x_out.at[f, pl.ds(half - plane, half)], middle.at[f], send_m.at[f], recv_m.at[f],
            device_id=(partner, col), device_id_type=MESH,
        )

    def send_x(f, carry):
        def send(at, carry):
            peer = row ^ at
            pltpu.make_async_remote_copy(
                x_out.at[f, peer], y_in.at[f, row], send_a.at[f], recv_a.at[f],
                device_id=(peer, col), device_id_type=MESH,
            ).start()
            return carry

        return lax.fori_loop(1, half, send, carry)

    def pass_on(f):
        pltpu.make_async_copy(middle.at[f], middle.at[f], recv_m.at[f]).wait()

        def send(at, carry):
            peer = row ^ at
            pltpu.make_async_remote_copy(
                middle.at[f, place ^ at], y_in.at[f, partner], send_a.at[f], recv_a.at[f],
                device_id=(peer, col), device_id_type=MESH,
            ).start()
            return carry

        lax.fori_loop(1, half, send, 0)
        y_in[f, partner] = middle[f, place]

    def stage_y(f):
        others = y_in.at[f, pl.ds(0, rows - 2)]
        pltpu.make_async_copy(others, others, recv_a.at[f]).wait()
        columns = []
        for pair in range(pairs):
            even = y_in[f, :, 2 * pair, :]
            odd = y_in[f, :, 2 * pair + 1, :]
            planes = join(even[:, :128], odd[:, :128]) + join(even[:, 128:], odd[:, 128:])
            columns.append(jnp.concatenate(planes, axis=0))
        lines = jnp.concatenate(columns, axis=1)
        modes = product((table_y[0], table_y[1]), split(lines), (((1,), (0,))))
        for pair in range(pairs):
            block = modes[:, 128 * pair : 128 * (pair + 1)].reshape(cols, share_k, 128)
            for at in range(cols):
                y_out[f, at, pair] = block[at]
        z_in[f, col] = y_out[f, col]

        def send(at, carry):
            peer = col ^ at
            pltpu.make_async_remote_copy(
                y_out.at[f, peer], z_in.at[f, col], send_b.at[f], recv_b.at[f],
                device_id=(row, peer), device_id_type=MESH,
            ).start()
            return carry

        lax.fori_loop(1, cols, send, 0)

    compute_x(relayed[0])
    pl.semaphore_wait(barrier, 7)
    relay_of(relayed[0], 0).start()
    relay_of(relayed[0], 1).start()
    signal(token.at[0], ring(1), ring(-1))
    signal(token.at[1], beside_x(1), beside_x(-1))
    compute_x(relayed[1])
    relay_of(relayed[1], 0).start()
    relay_of(relayed[1], 1).start()
    pl.semaphore_wait(token.at[0], 2)
    pl.semaphore_wait(token.at[1], 2)
    signal(token.at[2], ring(1), ring(-1))
    signal(token.at[3], beside_x(-1))
    compute_x(straight[0])
    pl.semaphore_wait(token.at[2], 2)
    pl.semaphore_wait(token.at[3], 1)
    signal(token.at[4], ring(1))
    signal(token.at[5], beside_y(1), beside_y(-1))
    compute_x(straight[1])
    pl.semaphore_wait(token.at[4], 1)
    for f in straight:
        across(f).start()
    pl.semaphore_wait(token.at[5], 2)
    signal(token.at[6], beside_y(-1))
    pl.semaphore_wait(token.at[6], 1)
    lax.fori_loop(0, fields, send_x, 0)
    for f in relayed:
        for way in range(2):
            relay_of(f, way).wait_recv()
            forward_of(f, way).start()
    for copy in rest[1:]:
        copy.wait()

    def second(f, carry):
        pass_on(f)
        stage_y(f)
        return carry

    lax.fori_loop(0, fields, second, 0)

    here = lax.broadcasted_iota(jnp.int32, (share_k, 256), 0) + col * share_k
    there = lax.broadcasted_iota(jnp.int32, (share_k, 256), 1)
    part_y = jnp.sum(jnp.where(here == there, symbol_y[...], 0.0), axis=1, keepdims=True)
    symbol_yz = part_y + symbol_z[...]
    lane_x = lax.broadcasted_iota(jnp.int32, symbol_x.shape, 1) - row * share_x

    def stage_z(f, carry):
        others = z_in.at[f, pl.ds(0, cols - 1)]
        pltpu.make_async_copy(others, others, recv_b.at[f]).wait()
        lines = []
        for pair in range(pairs):
            even0, odd0 = join(z_in[f, 0, pair], z_in[f, 1, pair])
            even1, odd1 = join(z_in[f, 2, pair], z_in[f, 3, pair])
            lines.append(jnp.concatenate([even0, even1], axis=1))
            lines.append(jnp.concatenate([odd0, odd1], axis=1))
        lines = jnp.concatenate(lines, axis=0)
        modes = product(split(lines), (table_z[0], table_z[1]), (((1,), (0,))))
        for x in range(share_x):
            part_x = jnp.sum(jnp.where(lane_x == x, symbol_x[...], 0.0), axis=1, keepdims=True)
            out[f, x] = modes[share_k * x : share_k * (x + 1)] / (part_x + symbol_yz)
        return carry

    lax.fori_loop(0, fields, stage_z, 0)

    def drain(f, carry):
        sent = x_out.at[f, pl.ds(0, rows - 2)]
        pltpu.make_async_copy(sent, sent, send_a.at[f]).wait()
        sent = y_out.at[f, pl.ds(0, cols - 1)]
        pltpu.make_async_copy(sent, sent, send_b.at[f]).wait()
        return carry

    lax.fori_loop(0, fields, drain, 0)
    for f in straight:
        across(f).wait_send()
    for f in relayed:
        for way in range(2):
            relay_of(f, way).wait_send()
            forward_of(f, way).wait_send()


def on_device(rows, cols, tables, species, symbol_x, symbol_y, symbol_z):
    fields, grid_x, share_y, share_z = species.shape
    grid_y, grid_z = share_y * rows, share_z * cols
    share_x, share_k = grid_x // rows, grid_y // cols
    field = species.transpose(0, 2, 3, 1).reshape(fields, share_y * share_z, grid_x)
    hbm = pl.BlockSpec(memory_space=pltpu.HBM)
    return pl.pallas_call(
        functools.partial(kernel, rows, cols),
        out_shape=pltpu.VMEM((fields, share_x, share_k, grid_z), jnp.float32),
        in_specs=[hbm] * 7,
        out_specs=pl.BlockSpec(memory_space=pltpu.VMEM),
        scratch_shapes=[
            pltpu.VMEM(field.shape, jnp.float32),
            *(pltpu.VMEM(table.shape, table.dtype) for table in tables),
            pltpu.VMEM((1, grid_x), jnp.float32),
            pltpu.VMEM((1, grid_y), jnp.float32),
            pltpu.VMEM((1, grid_z), jnp.float32),
            pltpu.VMEM((fields, rows, share_x, share_y * share_z), jnp.float32),
            pltpu.VMEM((fields // 2, 2, rows // 4, share_x, share_y * share_z), jnp.float32),
            pltpu.VMEM((fields, rows // 2, share_x, share_y * share_z), jnp.float32),
            pltpu.VMEM((fields, rows, share_x, share_y * share_z), jnp.float32),
            pltpu.VMEM((fields, cols, share_x // 2, share_k, 2 * share_z), jnp.float32),
            pltpu.VMEM((fields, cols, share_x // 2, share_k, 2 * share_z), jnp.float32),
            pltpu.SemaphoreType.REGULAR((7,)),
            pltpu.SemaphoreType.DMA((fields // 2, 2)),
            pltpu.SemaphoreType.DMA((fields // 2, 2)),
            pltpu.SemaphoreType.DMA((fields // 2, 2)),
            pltpu.SemaphoreType.DMA((fields,)),
            pltpu.SemaphoreType.DMA((fields,)),
            pltpu.SemaphoreType.DMA((fields,)),
            pltpu.SemaphoreType.DMA((fields,)),
            pltpu.SemaphoreType.DMA((fields,)),
            pltpu.SemaphoreType.DMA((fields,)),
            pltpu.SemaphoreType.DMA((fields,)),
            pltpu.SemaphoreType.DMA((6,)),
        ],
        compiler_params=pltpu.CompilerParams(
            collective_id=0, has_side_effects=True, vmem_limit_bytes=20 * 2**20
        ),
    )(*(pltpu.with_memory_space_constraint(a, pltpu.HBM) for a in (field, *tables, symbol_x[None], symbol_y[None], symbol_z[None])))


def solution(mesh):
    rows, cols = mesh.shape["row"], mesh.shape["col"]

    def whole(species, symbol_x, symbol_y, symbol_z):
        _, grid_x, grid_y, grid_z = species.shape
        share_y = grid_y // rows
        order = np.arange(grid_y).reshape(rows, share_y).T.reshape(-1)
        tables = (
            jnp.asarray(halves_of(transform_table(grid_x))),
            jnp.asarray(halves_of(transform_table(grid_y)[:, order])),
            jnp.asarray(halves_of(transform_table(grid_z))),
        )
        return jax.shard_map(
            functools.partial(on_device, rows, cols),
            mesh=mesh,
            in_specs=((P(), P(), P()), P(None, None, "row", "col"), P(), P(), P()),
            out_specs=P(None, "row", "col", None),
            check_vma=False,
        )(tables, species, symbol_x, symbol_y, symbol_z)

    return whole
```

```python
import functools
import math

import jax
import jax.numpy as jnp
import ml_dtypes
import numpy as np
from jax import lax
from jax.experimental import pallas as pl
from jax.experimental.pallas import tpu as pltpu
from jax.sharding import PartitionSpec as P

MESH = pl.DeviceIdType.MESH


def transform_table(count):
    rank = np.arange(count)
    step = (rank[:, None] + 1) * (rank[None, :] + 1) % (2 * count + 2)
    table = (np.sin(np.pi / (count + 1) * step) * (2.0 / (count + 1)) ** 0.5).astype(np.float32)
    return table


def halves_of(table):
    high = table.astype(ml_dtypes.bfloat16)
    low = (table - high.astype(np.float32)).astype(ml_dtypes.bfloat16)
    return np.stack([high, low])


def split(values):
    high = values.astype(jnp.bfloat16)
    return high, (values - high.astype(jnp.float32)).astype(jnp.bfloat16)


def product(left, right, dims):
    dot = functools.partial(
        lax.dot_general, dimension_numbers=(dims, ((), ())), preferred_element_type=jnp.float32
    )
    return dot(left[0], right[0]) + (dot(left[0], right[1]) + dot(left[1], right[0]))


def kernel(
    rows, cols,
    field_hbm, table_x_hbm, table_y_hbm, table_z_hbm, symbol_x_hbm, symbol_y_hbm, symbol_z_hbm,
    out,
    field, table_x, table_y, table_z, symbol_x, symbol_y, symbol_z,
    x_out, relay, middle, y_in, y_out, z_in,
    token, send_r, recv_r, send_w, recv_m, send_a, recv_a, send_b, recv_b, load_field, load_rest,
):
    fields = field.shape[0]
    row, col = lax.axis_index("row"), lax.axis_index("col")
    share_x = x_out.shape[2]
    share_k = z_in.shape[3]
    pairs = z_in.shape[2]

    barrier = pltpu.get_barrier_semaphore()

    half = rows // 2
    partner = row ^ half
    plane = row // half * half
    place = row - plane
    side = math.isqrt(half // 2)
    layers = 2 * cols
    layer = row // half * cols + col
    at_x, at_y = lax.rem(place // 2, side), place // (2 * side)

    def ring(step):
        there = lax.rem(layer + step + layers, layers)
        return place + there // cols * half, lax.rem(there, cols)

    def beside_x(step):
        return row + 2 * (lax.rem(at_x + step + side, side) - at_x), col

    def beside_y(step):
        return row + 2 * side * (lax.rem(at_y + step + side, side) - at_y), col

    def signal(semaphore, *devices):
        for device in devices:
            pl.semaphore_signal(semaphore, inc=1, device_id=device, device_id_type=MESH)

    loads = [pltpu.make_async_copy(field_hbm.at[f], field.at[f], load_field.at[f]) for f in range(fields)]
    rest = [
        pltpu.make_async_copy(source, target, load_rest.at[at])
        for at, (source, target) in enumerate((
            (table_x_hbm, table_x), (table_y_hbm, table_y), (table_z_hbm, table_z),
            (symbol_x_hbm, symbol_x), (symbol_y_hbm, symbol_y), (symbol_z_hbm, symbol_z),
        ))
    ]
    loads[0].start()
    rest[0].start()
    signal(
        barrier, ring(1), ring(-1), (row ^ 1, col),
        beside_x(1), beside_x(-1), beside_y(1), beside_y(-1),
    )
    for copy in loads[1:] + rest[1:]:
        copy.start()
    rest[0].wait()

    lane = lax.broadcasted_iota(jnp.int32, (1, 128), 1)
    low_half = lane < 64

    def join(first, second):
        return (
            jnp.where(low_half, first, pltpu.roll(second, 64, 1)),
            jnp.where(low_half, pltpu.roll(first, 64, 1), second),
        )

    def compute_x(f):
        pltpu.make_async_copy(field_hbm.at[f], field.at[f], load_field.at[f]).wait()
        modes = product((table_x[0], table_x[1]), split(field[f]), (((1,), (1,))))
        x_out[f] = modes.reshape(x_out.shape[1:])
        y_in[f, row] = x_out[f, row]

    def relay_of(f, way):
        return pltpu.make_async_remote_copy(
            x_out.at[f, pl.ds(half - plane + way * (half // 2), half // 2)],
            relay.at[f, way], send_r.at[f, way], recv_r.at[f, way],
            device_id=ring(1 - 2 * way), device_id_type=MESH,
        )

    def forward_of(f, way):
        return pltpu.make_async_remote_copy(
            relay.at[f, way], middle.at[f, pl.ds(way * (half // 2), half // 2)],
            send_w.at[f, way], recv_m.at[f],
            device_id=ring(3 - 6 * way), device_id_type=MESH,
        )

    def send_x(f, carry):
        def send(at, carry):
            peer = row ^ at
            pltpu.make_async_remote_copy(
                x_out.at[f, peer], y_in.at[f, row], send_a.at[f], recv_a.at[f],
                device_id=(peer, col), device_id_type=MESH,
            ).start()
            return carry

        return lax.fori_loop(1, half, send, carry)

    def pass_on(f):
        pltpu.make_async_copy(middle.at[f], middle.at[f], recv_m.at[f]).wait()

        def send(at, carry):
            peer = row ^ at
            pltpu.make_async_remote_copy(
                middle.at[f, place ^ at], y_in.at[f, partner], send_a.at[f], recv_a.at[f],
                device_id=(peer, col), device_id_type=MESH,
            ).start()
            return carry

        lax.fori_loop(1, half, send, 0)
        y_in[f, partner] = middle[f, place]

    def stage_y(f):
        others = y_in.at[f, pl.ds(0, rows - 2)]
        pltpu.make_async_copy(others, others, recv_a.at[f]).wait()
        columns = []
        for pair in range(pairs):
            even = y_in[f, :, 2 * pair, :]
            odd = y_in[f, :, 2 * pair + 1, :]
            planes = join(even[:, :128], odd[:, :128]) + join(even[:, 128:], odd[:, 128:])
            columns.append(jnp.concatenate(planes, axis=0))
        lines = jnp.concatenate(columns, axis=1)
        modes = product((table_y[0], table_y[1]), split(lines), (((1,), (0,))))
        for pair in range(pairs):
            block = modes[:, 128 * pair : 128 * (pair + 1)].reshape(cols, share_k, 128)
            for at in range(cols):
                y_out[f, at, pair] = block[at]
        z_in[f, col] = y_out[f, col]

        def send(at, carry):
            peer = col ^ at
            pltpu.make_async_remote_copy(
                y_out.at[f, peer], z_in.at[f, col], send_b.at[f], recv_b.at[f],
                device_id=(row, peer), device_id_type=MESH,
            ).start()
            return carry

        lax.fori_loop(1, cols, send, 0)

    def prepare(f):
        compute_x(f)
        relay_of(f, 0).start()
        relay_of(f, 1).start()

    compute_x(0)
    pl.semaphore_wait(barrier, 7)
    relay_of(0, 0).start()
    relay_of(0, 1).start()
    signal(token.at[0], ring(1), ring(-1))
    signal(token.at[1], beside_x(1), beside_x(-1))
    prepare(1)
    pl.semaphore_wait(token.at[0], 2)
    pl.semaphore_wait(token.at[1], 2)
    signal(token.at[2], ring(1), ring(-1))
    signal(token.at[3], beside_x(-1))
    prepare(2)
    pl.semaphore_wait(token.at[2], 2)
    pl.semaphore_wait(token.at[3], 1)
    signal(token.at[4], beside_y(1), beside_y(-1))
    prepare(3)
    pl.semaphore_wait(token.at[4], 2)
    signal(token.at[5], beside_y(-1))
    pl.semaphore_wait(token.at[5], 1)
    lax.fori_loop(0, fields, send_x, 0)
    for f in range(fields):
        for way in range(2):
            relay_of(f, way).wait_recv()
            forward_of(f, way).start()
    for copy in rest[1:]:
        copy.wait()

    def second(f, carry):
        pass_on(f)
        stage_y(f)
        return carry

    lax.fori_loop(0, fields, second, 0)

    here = lax.broadcasted_iota(jnp.int32, (share_k, 256), 0) + col * share_k
    there = lax.broadcasted_iota(jnp.int32, (share_k, 256), 1)
    part_y = jnp.sum(jnp.where(here == there, symbol_y[...], 0.0), axis=1, keepdims=True)
    symbol_yz = part_y + symbol_z[...]
    lane_x = lax.broadcasted_iota(jnp.int32, symbol_x.shape, 1) - row * share_x

    def stage_z(f, carry):
        others = z_in.at[f, pl.ds(0, cols - 1)]
        pltpu.make_async_copy(others, others, recv_b.at[f]).wait()
        lines = []
        for pair in range(pairs):
            even0, odd0 = join(z_in[f, 0, pair], z_in[f, 1, pair])
            even1, odd1 = join(z_in[f, 2, pair], z_in[f, 3, pair])
            lines.append(jnp.concatenate([even0, even1], axis=1))
            lines.append(jnp.concatenate([odd0, odd1], axis=1))
        lines = jnp.concatenate(lines, axis=0)
        modes = product(split(lines), (table_z[0], table_z[1]), (((1,), (0,))))
        for x in range(share_x):
            part_x = jnp.sum(jnp.where(lane_x == x, symbol_x[...], 0.0), axis=1, keepdims=True)
            out[f, x] = modes[share_k * x : share_k * (x + 1)] / (part_x + symbol_yz)
        return carry

    lax.fori_loop(0, fields, stage_z, 0)

    def drain(f, carry):
        sent = x_out.at[f, pl.ds(0, rows - 2)]
        pltpu.make_async_copy(sent, sent, send_a.at[f]).wait()
        sent = y_out.at[f, pl.ds(0, cols - 1)]
        pltpu.make_async_copy(sent, sent, send_b.at[f]).wait()
        return carry

    lax.fori_loop(0, fields, drain, 0)
    for f in range(fields):
        for way in range(2):
            relay_of(f, way).wait_send()
            forward_of(f, way).wait_send()


def on_device(rows, cols, tables, species, symbol_x, symbol_y, symbol_z):
    fields, grid_x, share_y, share_z = species.shape
    grid_y, grid_z = share_y * rows, share_z * cols
    share_x, share_k = grid_x // rows, grid_y // cols
    field = species.transpose(0, 2, 3, 1).reshape(fields, share_y * share_z, grid_x)
    hbm = pl.BlockSpec(memory_space=pltpu.HBM)
    return pl.pallas_call(
        functools.partial(kernel, rows, cols),
        out_shape=pltpu.VMEM((fields, share_x, share_k, grid_z), jnp.float32),
        in_specs=[hbm] * 7,
        out_specs=pl.BlockSpec(memory_space=pltpu.VMEM),
        scratch_shapes=[
            pltpu.VMEM(field.shape, jnp.float32),
            *(pltpu.VMEM(table.shape, table.dtype) for table in tables),
            pltpu.VMEM((1, grid_x), jnp.float32),
            pltpu.VMEM((1, grid_y), jnp.float32),
            pltpu.VMEM((1, grid_z), jnp.float32),
            pltpu.VMEM((fields, rows, share_x, share_y * share_z), jnp.float32),
            pltpu.VMEM((fields, 2, rows // 4, share_x, share_y * share_z), jnp.float32),
            pltpu.VMEM((fields, rows // 2, share_x, share_y * share_z), jnp.float32),
            pltpu.VMEM((fields, rows, share_x, share_y * share_z), jnp.float32),
            pltpu.VMEM((fields, cols, share_x // 2, share_k, 2 * share_z), jnp.float32),
            pltpu.VMEM((fields, cols, share_x // 2, share_k, 2 * share_z), jnp.float32),
            pltpu.SemaphoreType.REGULAR((6,)),
            pltpu.SemaphoreType.DMA((fields, 2)),
            pltpu.SemaphoreType.DMA((fields, 2)),
            pltpu.SemaphoreType.DMA((fields, 2)),
            pltpu.SemaphoreType.DMA((fields,)),
            pltpu.SemaphoreType.DMA((fields,)),
            pltpu.SemaphoreType.DMA((fields,)),
            pltpu.SemaphoreType.DMA((fields,)),
            pltpu.SemaphoreType.DMA((fields,)),
            pltpu.SemaphoreType.DMA((fields,)),
            pltpu.SemaphoreType.DMA((6,)),
        ],
        compiler_params=pltpu.CompilerParams(
            collective_id=0, has_side_effects=True, vmem_limit_bytes=20 * 2**20
        ),
    )(*(pltpu.with_memory_space_constraint(a, pltpu.HBM) for a in (field, *tables, symbol_x[None], symbol_y[None], symbol_z[None])))


def solution(mesh):
    rows, cols = mesh.shape["row"], mesh.shape["col"]

    def whole(species, symbol_x, symbol_y, symbol_z):
        _, grid_x, grid_y, grid_z = species.shape
        share_y = grid_y // rows
        order = np.arange(grid_y).reshape(rows, share_y).T.reshape(-1)
        tables = (
            jnp.asarray(halves_of(transform_table(grid_x))),
            jnp.asarray(halves_of(transform_table(grid_y)[:, order])),
            jnp.asarray(halves_of(transform_table(grid_z))),
        )
        return jax.shard_map(
            functools.partial(on_device, rows, cols),
            mesh=mesh,
            in_specs=((P(), P(), P()), P(None, None, "row", "col"), P(), P(), P()),
            out_specs=P(None, "row", "col", None),
            check_vma=False,
        )(tables, species, symbol_x, symbol_y, symbol_z)

    return whole
```

```python
import functools
import math

import jax
import jax.numpy as jnp
import ml_dtypes
import numpy as np
from jax import lax
from jax.experimental import pallas as pl
from jax.experimental.pallas import tpu as pltpu
from jax.sharding import PartitionSpec as P

MESH = pl.DeviceIdType.MESH


def transform_table(count):
    rank = np.arange(count)
    step = (rank[:, None] + 1) * (rank[None, :] + 1) % (2 * count + 2)
    table = (np.sin(np.pi / (count + 1) * step) * (2.0 / (count + 1)) ** 0.5).astype(np.float32)
    return table


def halves_of(table):
    high = table.astype(ml_dtypes.bfloat16)
    low = (table - high.astype(np.float32)).astype(ml_dtypes.bfloat16)
    return np.stack([high, low])


def split(values):
    high = values.astype(jnp.bfloat16)
    return high, (values - high.astype(jnp.float32)).astype(jnp.bfloat16)


def product(left, right, dims):
    dot = functools.partial(
        lax.dot_general, dimension_numbers=(dims, ((), ())), preferred_element_type=jnp.float32
    )
    return dot(left[0], right[0]) + (dot(left[0], right[1]) + dot(left[1], right[0]))


def join(first, second):
    low_half = lax.broadcasted_iota(jnp.int32, (1, 128), 1) < 64
    return (
        jnp.where(low_half, first, pltpu.roll(second, 64, 1)),
        jnp.where(low_half, pltpu.roll(first, 64, 1), second),
    )


def modes_of_z(blocks, table_z, pairs):
    lines = []
    for pair in pairs:
        even0, odd0 = join(blocks(0, pair), blocks(1, pair))
        even1, odd1 = join(blocks(2, pair), blocks(3, pair))
        lines.append(jnp.concatenate([even0, even1], axis=1))
        lines.append(jnp.concatenate([odd0, odd1], axis=1))
    lines = jnp.concatenate(lines, axis=0)
    return product(split(lines), (table_z[0], table_z[1]), (((1,), (0,))))


def finish(done, landed, table_z, symbol, out, staged, sems):
    fields = done.shape[0]
    share_x, share_k = symbol.shape[:2]
    copies = [pltpu.make_async_copy(done.at[f], out.at[f], sems.at[f]) for f in range(fields)]
    for copy in copies:
        copy.start()
    half = share_x // 2
    for at in range(2):
        modes = modes_of_z(
            lambda c, pair: landed[c, pair], table_z, range(at * half // 2, (at + 1) * half // 2)
        )
        for x in range(half):
            staged[at * half + x] = modes[share_k * x : share_k * (x + 1)] / symbol[at * half + x]
        part = pl.ds(at * half, half)
        copies.append(pltpu.make_async_copy(staged.at[part], out.at[fields, part], sems.at[fields + at]))
        copies[-1].start()
    for copy in copies:
        copy.wait()


def kernel(
    rows, cols,
    field_hbm, table_x_hbm, table_y_hbm, table_z_hbm, symbol_x_hbm, symbol_y_hbm, symbol_z_hbm,
    out, landed, table_z, symbol,
    field, table_x, table_y, symbol_x, symbol_y, symbol_z,
    x_out, relay, middle, y_in, y_out, z_in,
    token, send_r, recv_r, send_w, recv_m, send_a, recv_a, send_b, recv_b, load_field, load_rest,
):
    fields = field.shape[0]
    row, col = lax.axis_index("row"), lax.axis_index("col")
    share_x = x_out.shape[2]
    share_k = z_in.shape[3]
    pairs = z_in.shape[2]

    barrier = pltpu.get_barrier_semaphore()

    half = rows // 2
    partner = row ^ half
    plane = row // half * half
    place = row - plane
    side = math.isqrt(half // 2)
    layers = 2 * cols
    layer = row // half * cols + col
    at_x, at_y = lax.rem(place // 2, side), place // (2 * side)

    def ring(step):
        there = lax.rem(layer + step + layers, layers)
        return place + there // cols * half, lax.rem(there, cols)

    def beside_x(step):
        return row + 2 * (lax.rem(at_x + step + side, side) - at_x), col

    def beside_y(step):
        return row + 2 * side * (lax.rem(at_y + step + side, side) - at_y), col

    def signal(semaphore, *devices):
        for device in devices:
            pl.semaphore_signal(semaphore, inc=1, device_id=device, device_id_type=MESH)

    loads = [pltpu.make_async_copy(field_hbm.at[f], field.at[f], load_field.at[f]) for f in range(fields)]
    rest = [
        pltpu.make_async_copy(source, target, load_rest.at[at])
        for at, (source, target) in enumerate((
            (table_x_hbm, table_x), (table_y_hbm, table_y), (table_z_hbm, table_z),
            (symbol_x_hbm, symbol_x), (symbol_y_hbm, symbol_y), (symbol_z_hbm, symbol_z),
        ))
    ]
    loads[0].start()
    rest[0].start()
    signal(
        barrier, ring(1), ring(-1), (row ^ 1, col),
        beside_x(1), beside_x(-1), beside_y(1), beside_y(-1),
    )
    for copy in loads[1:] + rest[1:]:
        copy.start()
    rest[0].wait()

    def compute_x(f):
        pltpu.make_async_copy(field_hbm.at[f], field.at[f], load_field.at[f]).wait()
        modes = product((table_x[0], table_x[1]), split(field[f]), (((1,), (1,))))
        x_out[f] = modes.reshape(x_out.shape[1:])
        y_in[f, row] = x_out[f, row]

    def relay_of(f, way):
        return pltpu.make_async_remote_copy(
            x_out.at[f, pl.ds(half - plane + way * (half // 2), half // 2)],
            relay.at[f, way], send_r.at[f, way], recv_r.at[f, way],
            device_id=ring(1 - 2 * way), device_id_type=MESH,
        )

    def forward_of(f, way):
        return pltpu.make_async_remote_copy(
            relay.at[f, way], middle.at[f, pl.ds(way * (half // 2), half // 2)],
            send_w.at[f, way], recv_m.at[f],
            device_id=ring(3 - 6 * way), device_id_type=MESH,
        )

    def send_x(f, carry):
        def send(at, carry):
            peer = row ^ at
            pltpu.make_async_remote_copy(
                x_out.at[f, peer], y_in.at[f, row], send_a.at[f], recv_a.at[f],
                device_id=(peer, col), device_id_type=MESH,
            ).start()
            return carry

        return lax.fori_loop(1, half, send, carry)

    def pass_on(f):
        pltpu.make_async_copy(middle.at[f], middle.at[f], recv_m.at[f]).wait()

        def send(at, carry):
            peer = row ^ at
            pltpu.make_async_remote_copy(
                middle.at[f, place ^ at], y_in.at[f, partner], send_a.at[f], recv_a.at[f],
                device_id=(peer, col), device_id_type=MESH,
            ).start()
            return carry

        lax.fori_loop(1, half, send, 0)
        y_in[f, partner] = middle[f, place]

    def stage_y(f):
        others = y_in.at[f, pl.ds(0, rows - 2)]
        pltpu.make_async_copy(others, others, recv_a.at[f]).wait()
        columns = []
        for pair in range(pairs):
            even = y_in[f, :, 2 * pair, :]
            odd = y_in[f, :, 2 * pair + 1, :]
            planes = join(even[:, :128], odd[:, :128]) + join(even[:, 128:], odd[:, 128:])
            columns.append(jnp.concatenate(planes, axis=0))
        lines = jnp.concatenate(columns, axis=1)
        modes = product((table_y[0], table_y[1]), split(lines), (((1,), (0,))))
        for pair in range(pairs):
            block = modes[:, 128 * pair : 128 * (pair + 1)].reshape(cols, share_k, 128)
            for at in range(cols):
                y_out[f, at, pair] = block[at]
        z_in[f, col] = y_out[f, col]

        def send(at, carry):
            peer = col ^ at
            pltpu.make_async_remote_copy(
                y_out.at[f, peer], z_in.at[f, col], send_b.at[f], recv_b.at[f],
                device_id=(row, peer), device_id_type=MESH,
            ).start()
            return carry

        lax.fori_loop(1, cols, send, 0)

    def prepare(f):
        compute_x(f)
        relay_of(f, 0).start()
        relay_of(f, 1).start()

    compute_x(0)
    pl.semaphore_wait(barrier, 7)
    relay_of(0, 0).start()
    relay_of(0, 1).start()
    signal(token.at[0], ring(1), ring(-1))
    signal(token.at[1], beside_x(1), beside_x(-1))
    prepare(1)
    pl.semaphore_wait(token.at[0], 2)
    pl.semaphore_wait(token.at[1], 2)
    signal(token.at[2], ring(1), ring(-1))
    signal(token.at[3], beside_x(-1))
    prepare(2)
    pl.semaphore_wait(token.at[2], 2)
    pl.semaphore_wait(token.at[3], 1)
    signal(token.at[4], beside_y(1), beside_y(-1))
    prepare(3)
    pl.semaphore_wait(token.at[4], 2)
    signal(token.at[5], beside_y(-1))
    pl.semaphore_wait(token.at[5], 1)
    for f in range(fields):
        for way in range(2):
            relay_of(f, way).wait_recv()
            forward_of(f, way).start()
    lax.fori_loop(0, fields, send_x, 0)
    for copy in rest[1:]:
        copy.wait()

    def second(f, carry):
        pass_on(f)
        stage_y(f)
        return carry

    lax.fori_loop(0, fields, second, 0)

    here = lax.broadcasted_iota(jnp.int32, (share_k, 256), 0) + col * share_k
    there = lax.broadcasted_iota(jnp.int32, (share_k, 256), 1)
    part_y = jnp.sum(jnp.where(here == there, symbol_y[...], 0.0), axis=1, keepdims=True)
    symbol_yz = part_y + symbol_z[...]
    lane_x = lax.broadcasted_iota(jnp.int32, symbol_x.shape, 1) - row * share_x
    for x in range(share_x):
        part_x = jnp.sum(jnp.where(lane_x == x, symbol_x[...], 0.0), axis=1, keepdims=True)
        symbol[x] = part_x + symbol_yz

    def stage_z(f, carry):
        others = z_in.at[f, pl.ds(0, cols - 1)]
        pltpu.make_async_copy(others, others, recv_b.at[f]).wait()
        modes = modes_of_z(lambda c, pair: z_in[f, c, pair], table_z, range(pairs))
        for x in range(share_x):
            out[f, x] = modes[share_k * x : share_k * (x + 1)] / symbol[x]
        return carry

    lax.fori_loop(0, fields - 1, stage_z, 0)
    others = z_in.at[fields - 1, pl.ds(0, cols - 1)]
    pltpu.make_async_copy(others, others, recv_b.at[fields - 1]).wait()
    landed[...] = z_in[fields - 1]

    def drain(f, carry):
        sent = x_out.at[f, pl.ds(0, rows - 2)]
        pltpu.make_async_copy(sent, sent, send_a.at[f]).wait()
        sent = y_out.at[f, pl.ds(0, cols - 1)]
        pltpu.make_async_copy(sent, sent, send_b.at[f]).wait()
        return carry

    lax.fori_loop(0, fields, drain, 0)
    for f in range(fields):
        for way in range(2):
            relay_of(f, way).wait_send()
            forward_of(f, way).wait_send()


def on_device(rows, cols, tables, species, symbol_x, symbol_y, symbol_z):
    fields, grid_x, share_y, share_z = species.shape
    grid_y, grid_z = share_y * rows, share_z * cols
    share_x, share_k = grid_x // rows, grid_y // cols
    field = species.transpose(0, 2, 3, 1).reshape(fields, share_y * share_z, grid_x)
    hbm = pl.BlockSpec(memory_space=pltpu.HBM)
    done, landed, table_z, symbol = pl.pallas_call(
        functools.partial(kernel, rows, cols),
        out_shape=(
            pltpu.VMEM((fields - 1, share_x, share_k, grid_z), jnp.float32),
            pltpu.VMEM((cols, share_x // 2, share_k, 2 * share_z), jnp.float32),
            pltpu.VMEM(tables[2].shape, tables[2].dtype),
            pltpu.VMEM((share_x, share_k, grid_z), jnp.float32),
        ),
        in_specs=[hbm] * 7,
        out_specs=(pl.BlockSpec(memory_space=pltpu.VMEM),) * 4,
        scratch_shapes=[
            pltpu.VMEM(field.shape, jnp.float32),
            *(pltpu.VMEM(table.shape, table.dtype) for table in tables[:2]),
            pltpu.VMEM((1, grid_x), jnp.float32),
            pltpu.VMEM((1, grid_y), jnp.float32),
            pltpu.VMEM((1, grid_z), jnp.float32),
            pltpu.VMEM((fields, rows, share_x, share_y * share_z), jnp.float32),
            pltpu.VMEM((fields, 2, rows // 4, share_x, share_y * share_z), jnp.float32),
            pltpu.VMEM((fields, rows // 2, share_x, share_y * share_z), jnp.float32),
            pltpu.VMEM((fields, rows, share_x, share_y * share_z), jnp.float32),
            pltpu.VMEM((fields, cols, share_x // 2, share_k, 2 * share_z), jnp.float32),
            pltpu.VMEM((fields, cols, share_x // 2, share_k, 2 * share_z), jnp.float32),
            pltpu.SemaphoreType.REGULAR((6,)),
            pltpu.SemaphoreType.DMA((fields, 2)),
            pltpu.SemaphoreType.DMA((fields, 2)),
            pltpu.SemaphoreType.DMA((fields, 2)),
            pltpu.SemaphoreType.DMA((fields,)),
            pltpu.SemaphoreType.DMA((fields,)),
            pltpu.SemaphoreType.DMA((fields,)),
            pltpu.SemaphoreType.DMA((fields,)),
            pltpu.SemaphoreType.DMA((fields,)),
            pltpu.SemaphoreType.DMA((fields,)),
            pltpu.SemaphoreType.DMA((6,)),
        ],
        compiler_params=pltpu.CompilerParams(
            collective_id=0, has_side_effects=True, vmem_limit_bytes=20 * 2**20
        ),
    )(*(pltpu.with_memory_space_constraint(a, pltpu.HBM) for a in (field, *tables, symbol_x[None], symbol_y[None], symbol_z[None])))
    vmem = pl.BlockSpec(memory_space=pltpu.VMEM)
    return pl.pallas_call(
        finish,
        out_shape=jax.ShapeDtypeStruct((fields, share_x, share_k, grid_z), jnp.float32),
        in_specs=[vmem] * 4,
        out_specs=pl.BlockSpec(memory_space=pltpu.HBM),
        scratch_shapes=[
            pltpu.VMEM((share_x, share_k, grid_z), jnp.float32),
            pltpu.SemaphoreType.DMA((fields + 1,)),
        ],
        compiler_params=pltpu.CompilerParams(vmem_limit_bytes=8 * 2**20),
    )(done, landed, table_z, symbol)


def solution(mesh):
    rows, cols = mesh.shape["row"], mesh.shape["col"]

    def whole(species, symbol_x, symbol_y, symbol_z):
        _, grid_x, grid_y, grid_z = species.shape
        share_y = grid_y // rows
        order = np.arange(grid_y).reshape(rows, share_y).T.reshape(-1)
        tables = (
            jnp.asarray(halves_of(transform_table(grid_x))),
            jnp.asarray(halves_of(transform_table(grid_y)[:, order])),
            jnp.asarray(halves_of(transform_table(grid_z))),
        )
        return jax.shard_map(
            functools.partial(on_device, rows, cols),
            mesh=mesh,
            in_specs=((P(), P(), P()), P(None, None, "row", "col"), P(), P(), P()),
            out_specs=P(None, "row", "col", None),
            check_vma=False,
        )(tables, species, symbol_x, symbol_y, symbol_z)

    return whole
```

```python
import functools
import math

import jax
import jax.numpy as jnp
import ml_dtypes
import numpy as np
from jax import lax
from jax.experimental import pallas as pl
from jax.experimental.pallas import tpu as pltpu
from jax.sharding import PartitionSpec as P

MESH = pl.DeviceIdType.MESH


def transform_table(count):
    rank = np.arange(count)
    step = (rank[:, None] + 1) * (rank[None, :] + 1) % (2 * count + 2)
    table = (np.sin(np.pi / (count + 1) * step) * (2.0 / (count + 1)) ** 0.5).astype(np.float32)
    return table


def halves_of(table):
    high = table.astype(ml_dtypes.bfloat16)
    low = (table - high.astype(np.float32)).astype(ml_dtypes.bfloat16)
    return np.stack([high, low])


def split(values):
    high = values.astype(jnp.bfloat16)
    return high, (values - high.astype(jnp.float32)).astype(jnp.bfloat16)


def product(left, right, dims):
    dot = functools.partial(
        lax.dot_general, dimension_numbers=(dims, ((), ())), preferred_element_type=jnp.float32
    )
    return dot(left[0], right[0]) + (dot(left[0], right[1]) + dot(left[1], right[0]))


def join(first, second):
    low_half = lax.broadcasted_iota(jnp.int32, (1, 128), 1) < 64
    return (
        jnp.where(low_half, first, pltpu.roll(second, 64, 1)),
        jnp.where(low_half, pltpu.roll(first, 64, 1), second),
    )


def modes_of_z(blocks, table_z, pairs):
    lines = []
    for pair in pairs:
        even0, odd0 = join(blocks(0, pair), blocks(1, pair))
        even1, odd1 = join(blocks(2, pair), blocks(3, pair))
        lines.append(jnp.concatenate([even0, even1], axis=1))
        lines.append(jnp.concatenate([odd0, odd1], axis=1))
    lines = jnp.concatenate(lines, axis=0)
    return product(split(lines), (table_z[0], table_z[1]), (((1,), (0,))))


def finish(done, landed, table_z, symbol, out, staged, sems):
    fields = done.shape[0]
    share_x, share_k = symbol.shape[:2]
    copies = [pltpu.make_async_copy(done.at[f], out.at[f], sems.at[f]) for f in range(fields)]
    for copy in copies:
        copy.start()
    half = share_x // 2
    for at in range(2):
        modes = modes_of_z(
            lambda c, pair: landed[c, pair], table_z, range(at * half // 2, (at + 1) * half // 2)
        )
        for x in range(half):
            staged[at * half + x] = modes[share_k * x : share_k * (x + 1)] / symbol[at * half + x]
        part = pl.ds(at * half, half)
        copies.append(pltpu.make_async_copy(staged.at[part], out.at[fields, part], sems.at[fields + at]))
        copies[-1].start()
    for copy in copies:
        copy.wait()


def kernel(
    rows, cols,
    field_hbm, table_x_hbm, table_y_hbm, table_z_hbm, symbol_x_hbm, symbol_y_hbm, symbol_z_hbm,
    out, landed, table_z, symbol,
    field, table_x, table_y, symbol_x, symbol_y, symbol_z,
    x_out, relay, middle, y_in, y_out, z_in,
    token, send_r, recv_r, send_w, recv_m, send_a, recv_a, send_b, recv_b, load_field, load_rest,
):
    fields = field.shape[0]
    row, col = lax.axis_index("row"), lax.axis_index("col")
    share_x = x_out.shape[2]
    share_k = z_in.shape[3]
    pairs = z_in.shape[2]

    barrier = pltpu.get_barrier_semaphore()

    half = rows // 2
    partner = row ^ half
    plane = row // half * half
    place = row - plane
    side = math.isqrt(half // 2)
    layers = 2 * cols
    layer = row // half * cols + col
    at_x, at_y = lax.rem(place // 2, side), place // (2 * side)

    def ring(step):
        there = lax.rem(layer + step + layers, layers)
        return place + there // cols * half, lax.rem(there, cols)

    def beside_x(step):
        return row + 2 * (lax.rem(at_x + step + side, side) - at_x), col

    def beside_y(step):
        return row + 2 * side * (lax.rem(at_y + step + side, side) - at_y), col

    def signal(semaphore, *devices):
        for device in devices:
            pl.semaphore_signal(semaphore, inc=1, device_id=device, device_id_type=MESH)

    loads = [pltpu.make_async_copy(field_hbm.at[f], field.at[f], load_field.at[f]) for f in range(fields)]
    rest = [
        pltpu.make_async_copy(source, target, load_rest.at[at])
        for at, (source, target) in enumerate((
            (table_x_hbm, table_x), (table_y_hbm, table_y), (table_z_hbm, table_z),
            (symbol_x_hbm, symbol_x), (symbol_y_hbm, symbol_y), (symbol_z_hbm, symbol_z),
        ))
    ]
    loads[0].start()
    rest[0].start()
    signal(
        barrier, ring(1), ring(-1),
        beside_x(1), beside_x(-1), beside_y(1), beside_y(-1),
    )
    core = lax.rem(place, 2)

    @pl.when(core == 0)
    def _():
        signal(barrier, (row ^ 1, col))

    for copy in loads[1:] + rest[1:]:
        copy.start()
    rest[0].wait()

    def compute_x(f):
        pltpu.make_async_copy(field_hbm.at[f], field.at[f], load_field.at[f]).wait()
        modes = product((table_x[0], table_x[1]), split(field[f]), (((1,), (1,))))
        x_out[f] = modes.reshape(x_out.shape[1:])
        y_in[f, row] = x_out[f, row]

    def relay_of(f, way):
        return pltpu.make_async_remote_copy(
            x_out.at[f, pl.ds(half - plane + way * (half // 2), half // 2)],
            relay.at[f, way], send_r.at[f, way], recv_r.at[f, way],
            device_id=ring(1 - 2 * way), device_id_type=MESH,
        )

    def forward_of(f, way):
        return pltpu.make_async_remote_copy(
            relay.at[f, way], middle.at[f, pl.ds(way * (half // 2), half // 2)],
            send_w.at[f, way], recv_m.at[f],
            device_id=ring(3 - 6 * way), device_id_type=MESH,
        )

    def send_x(f, carry):
        def send(at, carry):
            peer = row ^ at
            pltpu.make_async_remote_copy(
                x_out.at[f, peer], y_in.at[f, row], send_a.at[f], recv_a.at[f],
                device_id=(peer, col), device_id_type=MESH,
            ).start()
            return carry

        return lax.fori_loop(1, half, send, carry)

    def pass_on(f):
        pltpu.make_async_copy(middle.at[f], middle.at[f], recv_m.at[f]).wait()

        def send(at, carry):
            peer = row ^ at
            pltpu.make_async_remote_copy(
                middle.at[f, place ^ at], y_in.at[f, partner], send_a.at[f], recv_a.at[f],
                device_id=(peer, col), device_id_type=MESH,
            ).start()
            return carry

        lax.fori_loop(1, half, send, 0)
        y_in[f, partner] = middle[f, place]

    def stage_y(f):
        others = y_in.at[f, pl.ds(0, rows - 2)]
        pltpu.make_async_copy(others, others, recv_a.at[f]).wait()
        columns = []
        for pair in range(pairs):
            even = y_in[f, :, 2 * pair, :]
            odd = y_in[f, :, 2 * pair + 1, :]
            planes = join(even[:, :128], odd[:, :128]) + join(even[:, 128:], odd[:, 128:])
            columns.append(jnp.concatenate(planes, axis=0))
        lines = jnp.concatenate(columns, axis=1)
        modes = product((table_y[0], table_y[1]), split(lines), (((1,), (0,))))
        for pair in range(pairs):
            block = modes[:, 128 * pair : 128 * (pair + 1)].reshape(cols, share_k, 128)
            for at in range(cols):
                y_out[f, at, pair] = block[at]
        z_in[f, col] = y_out[f, col]

        def send(at, carry):
            peer = col ^ at
            pltpu.make_async_remote_copy(
                y_out.at[f, peer], z_in.at[f, col], send_b.at[f], recv_b.at[f],
                device_id=(row, peer), device_id_type=MESH,
            ).start()
            return carry

        lax.fori_loop(1, cols, send, 0)

    def prepare(f):
        compute_x(f)
        relay_of(f, 0).start()
        relay_of(f, 1).start()

    compute_x(0)
    pl.semaphore_wait(barrier, 6 + core)
    relay_of(0, 0).start()
    relay_of(0, 1).start()
    signal(token.at[0], ring(1), ring(-1))

    @pl.when(core == 1)
    def _():
        signal(token.at[6], (row ^ 1, col))

    prepare(1)

    @pl.when(core == 0)
    def _():
        pl.semaphore_wait(token.at[6], 1)

    signal(token.at[1], beside_x(1), beside_x(-1))
    pl.semaphore_wait(token.at[0], 2)
    pl.semaphore_wait(token.at[1], 2)
    signal(token.at[2], ring(1), ring(-1))
    signal(token.at[3], beside_x(-1))
    prepare(2)
    pl.semaphore_wait(token.at[2], 2)
    pl.semaphore_wait(token.at[3], 1)
    signal(token.at[4], beside_y(1), beside_y(-1))
    prepare(3)
    pl.semaphore_wait(token.at[4], 2)
    signal(token.at[5], beside_y(-1))
    for f in range(fields):
        for way in range(2):
            relay_of(f, way).wait_recv()
            forward_of(f, way).start()
    pl.semaphore_wait(token.at[5], 1)
    lax.fori_loop(0, fields, send_x, 0)
    for copy in rest[1:]:
        copy.wait()

    def second(f, carry):
        pass_on(f)
        stage_y(f)
        return carry

    lax.fori_loop(0, fields, second, 0)

    here = lax.broadcasted_iota(jnp.int32, (share_k, 256), 0) + col * share_k
    there = lax.broadcasted_iota(jnp.int32, (share_k, 256), 1)
    part_y = jnp.sum(jnp.where(here == there, symbol_y[...], 0.0), axis=1, keepdims=True)
    symbol_yz = part_y + symbol_z[...]
    lane_x = lax.broadcasted_iota(jnp.int32, symbol_x.shape, 1) - row * share_x
    for x in range(share_x):
        part_x = jnp.sum(jnp.where(lane_x == x, symbol_x[...], 0.0), axis=1, keepdims=True)
        symbol[x] = part_x + symbol_yz

    def stage_z(f, carry):
        others = z_in.at[f, pl.ds(0, cols - 1)]
        pltpu.make_async_copy(others, others, recv_b.at[f]).wait()
        modes = modes_of_z(lambda c, pair: z_in[f, c, pair], table_z, range(pairs))
        for x in range(share_x):
            out[f, x] = modes[share_k * x : share_k * (x + 1)] / symbol[x]
        return carry

    lax.fori_loop(0, fields - 1, stage_z, 0)
    others = z_in.at[fields - 1, pl.ds(0, cols - 1)]
    pltpu.make_async_copy(others, others, recv_b.at[fields - 1]).wait()
    landed[...] = z_in[fields - 1]

    def drain(f, carry):
        sent = x_out.at[f, pl.ds(0, rows - 2)]
        pltpu.make_async_copy(sent, sent, send_a.at[f]).wait()
        sent = y_out.at[f, pl.ds(0, cols - 1)]
        pltpu.make_async_copy(sent, sent, send_b.at[f]).wait()
        return carry

    lax.fori_loop(0, fields, drain, 0)
    for f in range(fields):
        for way in range(2):
            relay_of(f, way).wait_send()
            forward_of(f, way).wait_send()


def on_device(rows, cols, tables, species, symbol_x, symbol_y, symbol_z):
    fields, grid_x, share_y, share_z = species.shape
    grid_y, grid_z = share_y * rows, share_z * cols
    share_x, share_k = grid_x // rows, grid_y // cols
    field = species.transpose(0, 2, 3, 1).reshape(fields, share_y * share_z, grid_x)
    hbm = pl.BlockSpec(memory_space=pltpu.HBM)
    done, landed, table_z, symbol = pl.pallas_call(
        functools.partial(kernel, rows, cols),
        out_shape=(
            pltpu.VMEM((fields - 1, share_x, share_k, grid_z), jnp.float32),
            pltpu.VMEM((cols, share_x // 2, share_k, 2 * share_z), jnp.float32),
            pltpu.VMEM(tables[2].shape, tables[2].dtype),
            pltpu.VMEM((share_x, share_k, grid_z), jnp.float32),
        ),
        in_specs=[hbm] * 7,
        out_specs=(pl.BlockSpec(memory_space=pltpu.VMEM),) * 4,
        scratch_shapes=[
            pltpu.VMEM(field.shape, jnp.float32),
            *(pltpu.VMEM(table.shape, table.dtype) for table in tables[:2]),
            pltpu.VMEM((1, grid_x), jnp.float32),
            pltpu.VMEM((1, grid_y), jnp.float32),
            pltpu.VMEM((1, grid_z), jnp.float32),
            pltpu.VMEM((fields, rows, share_x, share_y * share_z), jnp.float32),
            pltpu.VMEM((fields, 2, rows // 4, share_x, share_y * share_z), jnp.float32),
            pltpu.VMEM((fields, rows // 2, share_x, share_y * share_z), jnp.float32),
            pltpu.VMEM((fields, rows, share_x, share_y * share_z), jnp.float32),
            pltpu.VMEM((fields, cols, share_x // 2, share_k, 2 * share_z), jnp.float32),
            pltpu.VMEM((fields, cols, share_x // 2, share_k, 2 * share_z), jnp.float32),
            pltpu.SemaphoreType.REGULAR((7,)),
            pltpu.SemaphoreType.DMA((fields, 2)),
            pltpu.SemaphoreType.DMA((fields, 2)),
            pltpu.SemaphoreType.DMA((fields, 2)),
            pltpu.SemaphoreType.DMA((fields,)),
            pltpu.SemaphoreType.DMA((fields,)),
            pltpu.SemaphoreType.DMA((fields,)),
            pltpu.SemaphoreType.DMA((fields,)),
            pltpu.SemaphoreType.DMA((fields,)),
            pltpu.SemaphoreType.DMA((fields,)),
            pltpu.SemaphoreType.DMA((6,)),
        ],
        compiler_params=pltpu.CompilerParams(
            collective_id=0, has_side_effects=True, vmem_limit_bytes=20 * 2**20
        ),
    )(*(pltpu.with_memory_space_constraint(a, pltpu.HBM) for a in (field, *tables, symbol_x[None], symbol_y[None], symbol_z[None])))
    vmem = pl.BlockSpec(memory_space=pltpu.VMEM)
    return pl.pallas_call(
        finish,
        out_shape=jax.ShapeDtypeStruct((fields, share_x, share_k, grid_z), jnp.float32),
        in_specs=[vmem] * 4,
        out_specs=pl.BlockSpec(memory_space=pltpu.HBM),
        scratch_shapes=[
            pltpu.VMEM((share_x, share_k, grid_z), jnp.float32),
            pltpu.SemaphoreType.DMA((fields + 1,)),
        ],
        compiler_params=pltpu.CompilerParams(vmem_limit_bytes=8 * 2**20),
    )(done, landed, table_z, symbol)


def solution(mesh):
    rows, cols = mesh.shape["row"], mesh.shape["col"]

    def whole(species, symbol_x, symbol_y, symbol_z):
        _, grid_x, grid_y, grid_z = species.shape
        share_y = grid_y // rows
        order = np.arange(grid_y).reshape(rows, share_y).T.reshape(-1)
        tables = (
            jnp.asarray(halves_of(transform_table(grid_x))),
            jnp.asarray(halves_of(transform_table(grid_y)[:, order])),
            jnp.asarray(halves_of(transform_table(grid_z))),
        )
        return jax.shard_map(
            functools.partial(on_device, rows, cols),
            mesh=mesh,
            in_specs=((P(), P(), P()), P(None, None, "row", "col"), P(), P(), P()),
            out_specs=P(None, "row", "col", None),
            check_vma=False,
        )(tables, species, symbol_x, symbol_y, symbol_z)

    return whole
```

```python
import functools
import math

import jax
import jax.numpy as jnp
import ml_dtypes
import numpy as np
from jax import lax
from jax.experimental import pallas as pl
from jax.experimental.pallas import tpu as pltpu
from jax.sharding import PartitionSpec as P

MESH = pl.DeviceIdType.MESH


def transform_table(count):
    rank = np.arange(count)
    step = (rank[:, None] + 1) * (rank[None, :] + 1) % (2 * count + 2)
    table = (np.sin(np.pi / (count + 1) * step) * (2.0 / (count + 1)) ** 0.5).astype(np.float32)
    return table


def halves_of(table):
    high = table.astype(ml_dtypes.bfloat16)
    low = (table - high.astype(np.float32)).astype(ml_dtypes.bfloat16)
    return np.stack([high, low])


def split(values):
    high = values.astype(jnp.bfloat16)
    return high, (values - high.astype(jnp.float32)).astype(jnp.bfloat16)


def product(left, right, dims):
    dot = functools.partial(
        lax.dot_general, dimension_numbers=(dims, ((), ())), preferred_element_type=jnp.float32
    )
    return dot(left[0], right[0]) + (dot(left[0], right[1]) + dot(left[1], right[0]))


def join(first, second):
    low_half = lax.broadcasted_iota(jnp.int32, (1, 128), 1) < 64
    return (
        jnp.where(low_half, first, pltpu.roll(second, 64, 1)),
        jnp.where(low_half, pltpu.roll(first, 64, 1), second),
    )


def modes_of_z(blocks, table_z, pairs):
    lines = []
    for pair in pairs:
        even0, odd0 = join(blocks(0, pair), blocks(1, pair))
        even1, odd1 = join(blocks(2, pair), blocks(3, pair))
        lines.append(jnp.concatenate([even0, even1], axis=1))
        lines.append(jnp.concatenate([odd0, odd1], axis=1))
    lines = jnp.concatenate(lines, axis=0)
    return product(split(lines), (table_z[0], table_z[1]), (((1,), (0,))))


def finish(done, landed, table_z, symbol, out, staged, sems):
    fields = done.shape[0]
    share_x, share_k = symbol.shape[:2]
    copies = [pltpu.make_async_copy(done.at[f], out.at[f], sems.at[f]) for f in range(fields)]
    for copy in copies:
        copy.start()
    half = share_x // 2
    for at in range(2):
        modes = modes_of_z(
            lambda c, pair: landed[c, pair], table_z, range(at * half // 2, (at + 1) * half // 2)
        )
        for x in range(half):
            staged[at * half + x] = modes[share_k * x : share_k * (x + 1)] / symbol[at * half + x]
        part = pl.ds(at * half, half)
        copies.append(pltpu.make_async_copy(staged.at[part], out.at[fields, part], sems.at[fields + at]))
        copies[-1].start()
    for copy in copies:
        copy.wait()


def kernel(
    rows, cols,
    field_hbm, table_x_hbm, table_y_hbm, table_z_hbm, symbol_x_hbm, symbol_y_hbm, symbol_z_hbm,
    out, landed, table_z, symbol,
    field, table_x, table_y, symbol_x, symbol_y, symbol_z,
    x_out, relay, middle, y_in, y_out, z_in,
    token, send_r, recv_r, send_w, recv_m, send_a, recv_a, send_b, recv_b, load_field, load_rest,
):
    fields = field.shape[0]
    row, col = lax.axis_index("row"), lax.axis_index("col")
    share_x = x_out.shape[2]
    share_k = z_in.shape[3]
    pairs = z_in.shape[2]

    barrier = pltpu.get_barrier_semaphore()

    half = rows // 2
    partner = row ^ half
    plane = row // half * half
    place = row - plane
    side = math.isqrt(half // 2)
    layers = 2 * cols
    layer = row // half * cols + col
    at_x, at_y = lax.rem(place // 2, side), place // (2 * side)

    def ring(step):
        there = lax.rem(layer + step + layers, layers)
        return place + there // cols * half, lax.rem(there, cols)

    def beside_x(step):
        return row + 2 * (lax.rem(at_x + step + side, side) - at_x), col

    def beside_y(step):
        return row + 2 * side * (lax.rem(at_y + step + side, side) - at_y), col

    def signal(semaphore, *devices):
        for device in devices:
            pl.semaphore_signal(semaphore, inc=1, device_id=device, device_id_type=MESH)

    loads = [pltpu.make_async_copy(field_hbm.at[f], field.at[f], load_field.at[f]) for f in range(fields)]
    rest = [
        pltpu.make_async_copy(source, target, load_rest.at[at])
        for at, (source, target) in enumerate((
            (table_x_hbm, table_x), (table_y_hbm, table_y), (table_z_hbm, table_z),
            (symbol_x_hbm, symbol_x), (symbol_y_hbm, symbol_y), (symbol_z_hbm, symbol_z),
        ))
    ]
    signal(
        barrier, ring(1), ring(-1),
        beside_x(1), beside_x(-1), beside_y(1), beside_y(-1),
    )
    core = lax.rem(place, 2)

    @pl.when(core == 0)
    def _():
        signal(barrier, (row ^ 1, col))

    for copy in (loads[0], *rest[:1], *loads[1:], *rest[1:]):
        copy.start()
    rest[0].wait()

    def compute_x(f):
        pltpu.make_async_copy(field_hbm.at[f], field.at[f], load_field.at[f]).wait()
        modes = product((table_x[0], table_x[1]), split(field[f]), (((1,), (1,))))
        x_out[f] = modes.reshape(x_out.shape[1:])
        y_in[f, row] = x_out[f, row]

    def relay_of(f, way):
        return pltpu.make_async_remote_copy(
            x_out.at[f, pl.ds(half - plane + way * (half // 2), half // 2)],
            relay.at[f, way], send_r.at[f, way], recv_r.at[f, way],
            device_id=ring(1 - 2 * way), device_id_type=MESH,
        )

    def forward_of(f, way):
        return pltpu.make_async_remote_copy(
            relay.at[f, way], middle.at[f, pl.ds(way * (half // 2), half // 2)],
            send_w.at[f, way], recv_m.at[f],
            device_id=ring(3 - 6 * way), device_id_type=MESH,
        )

    def send_x(f, carry):
        def send(at, carry):
            peer = row ^ at
            pltpu.make_async_remote_copy(
                x_out.at[f, peer], y_in.at[f, row], send_a.at[f], recv_a.at[f],
                device_id=(peer, col), device_id_type=MESH,
            ).start()
            return carry

        return lax.fori_loop(1, half, send, carry)

    def pass_on(f):
        pltpu.make_async_copy(middle.at[f], middle.at[f], recv_m.at[f]).wait()

        def send(at, carry):
            peer = row ^ at
            pltpu.make_async_remote_copy(
                middle.at[f, place ^ at], y_in.at[f, partner], send_a.at[f], recv_a.at[f],
                device_id=(peer, col), device_id_type=MESH,
            ).start()
            return carry

        lax.fori_loop(1, half, send, 0)
        y_in[f, partner] = middle[f, place]

    def stage_y(f):
        others = y_in.at[f, pl.ds(0, rows - 2)]
        pltpu.make_async_copy(others, others, recv_a.at[f]).wait()
        columns = []
        for pair in range(pairs):
            even = y_in[f, :, 2 * pair, :]
            odd = y_in[f, :, 2 * pair + 1, :]
            planes = join(even[:, :128], odd[:, :128]) + join(even[:, 128:], odd[:, 128:])
            columns.append(jnp.concatenate(planes, axis=0))
        lines = jnp.concatenate(columns, axis=1)
        modes = product((table_y[0], table_y[1]), split(lines), (((1,), (0,))))
        for pair in range(pairs):
            block = modes[:, 128 * pair : 128 * (pair + 1)].reshape(cols, share_k, 128)
            for at in range(cols):
                y_out[f, at, pair] = block[at]
        z_in[f, col] = y_out[f, col]

        def send(at, carry):
            peer = col ^ at
            pltpu.make_async_remote_copy(
                y_out.at[f, peer], z_in.at[f, col], send_b.at[f], recv_b.at[f],
                device_id=(row, peer), device_id_type=MESH,
            ).start()
            return carry

        lax.fori_loop(1, cols, send, 0)

    def prepare(f):
        compute_x(f)
        relay_of(f, 0).start()
        relay_of(f, 1).start()

    compute_x(0)
    pl.semaphore_wait(barrier, 6 + core)
    relay_of(0, 0).start()
    relay_of(0, 1).start()
    signal(token.at[0], ring(1), ring(-1))

    @pl.when(core == 1)
    def _():
        signal(token.at[6], (row ^ 1, col))

    prepare(1)

    @pl.when(core == 0)
    def _():
        pl.semaphore_wait(token.at[6], 1)

    signal(token.at[1], beside_x(1), beside_x(-1))
    pl.semaphore_wait(token.at[0], 2)
    pl.semaphore_wait(token.at[1], 2)
    signal(token.at[2], ring(1), ring(-1))
    signal(token.at[3], beside_x(-1))
    prepare(2)
    pl.semaphore_wait(token.at[2], 2)
    pl.semaphore_wait(token.at[3], 1)
    signal(token.at[4], beside_y(1), beside_y(-1))
    prepare(3)
    pl.semaphore_wait(token.at[4], 2)
    signal(token.at[5], beside_y(-1))
    for f in range(fields):
        for way in range(2):
            relay_of(f, way).wait_recv()
            forward_of(f, way).start()
    pl.semaphore_wait(token.at[5], 1)
    lax.fori_loop(0, fields, send_x, 0)
    for copy in rest[1:]:
        copy.wait()

    def second(f, carry):
        pass_on(f)
        stage_y(f)
        return carry

    lax.fori_loop(0, fields, second, 0)

    here = lax.broadcasted_iota(jnp.int32, (share_k, 256), 0) + col * share_k
    there = lax.broadcasted_iota(jnp.int32, (share_k, 256), 1)
    part_y = jnp.sum(jnp.where(here == there, symbol_y[...], 0.0), axis=1, keepdims=True)
    symbol_yz = part_y + symbol_z[...]
    lane_x = lax.broadcasted_iota(jnp.int32, symbol_x.shape, 1) - row * share_x
    for x in range(share_x):
        part_x = jnp.sum(jnp.where(lane_x == x, symbol_x[...], 0.0), axis=1, keepdims=True)
        symbol[x] = part_x + symbol_yz

    def stage_z(f, carry):
        others = z_in.at[f, pl.ds(0, cols - 1)]
        pltpu.make_async_copy(others, others, recv_b.at[f]).wait()
        modes = modes_of_z(lambda c, pair: z_in[f, c, pair], table_z, range(pairs))
        for x in range(share_x):
            out[f, x] = modes[share_k * x : share_k * (x + 1)] / symbol[x]
        return carry

    lax.fori_loop(0, fields - 1, stage_z, 0)
    others = z_in.at[fields - 1, pl.ds(0, cols - 1)]
    pltpu.make_async_copy(others, others, recv_b.at[fields - 1]).wait()
    landed[...] = z_in[fields - 1]

    def drain(f, carry):
        sent = x_out.at[f, pl.ds(0, rows - 2)]
        pltpu.make_async_copy(sent, sent, send_a.at[f]).wait()
        sent = y_out.at[f, pl.ds(0, cols - 1)]
        pltpu.make_async_copy(sent, sent, send_b.at[f]).wait()
        return carry

    lax.fori_loop(0, fields, drain, 0)
    for f in range(fields):
        for way in range(2):
            relay_of(f, way).wait_send()
            forward_of(f, way).wait_send()


def on_device(rows, cols, tables, species, symbol_x, symbol_y, symbol_z):
    fields, grid_x, share_y, share_z = species.shape
    grid_y, grid_z = share_y * rows, share_z * cols
    share_x, share_k = grid_x // rows, grid_y // cols
    field = species.transpose(0, 2, 3, 1).reshape(fields, share_y * share_z, grid_x)
    hbm = pl.BlockSpec(memory_space=pltpu.HBM)
    done, landed, table_z, symbol = pl.pallas_call(
        functools.partial(kernel, rows, cols),
        out_shape=(
            pltpu.VMEM((fields - 1, share_x, share_k, grid_z), jnp.float32),
            pltpu.VMEM((cols, share_x // 2, share_k, 2 * share_z), jnp.float32),
            pltpu.VMEM(tables[2].shape, tables[2].dtype),
            pltpu.VMEM((share_x, share_k, grid_z), jnp.float32),
        ),
        in_specs=[hbm] * 7,
        out_specs=(pl.BlockSpec(memory_space=pltpu.VMEM),) * 4,
        scratch_shapes=[
            pltpu.VMEM(field.shape, jnp.float32),
            *(pltpu.VMEM(table.shape, table.dtype) for table in tables[:2]),
            pltpu.VMEM((1, grid_x), jnp.float32),
            pltpu.VMEM((1, grid_y), jnp.float32),
            pltpu.VMEM((1, grid_z), jnp.float32),
            pltpu.VMEM((fields, rows, share_x, share_y * share_z), jnp.float32),
            pltpu.VMEM((fields, 2, rows // 4, share_x, share_y * share_z), jnp.float32),
            pltpu.VMEM((fields, rows // 2, share_x, share_y * share_z), jnp.float32),
            pltpu.VMEM((fields, rows, share_x, share_y * share_z), jnp.float32),
            pltpu.VMEM((fields, cols, share_x // 2, share_k, 2 * share_z), jnp.float32),
            pltpu.VMEM((fields, cols, share_x // 2, share_k, 2 * share_z), jnp.float32),
            pltpu.SemaphoreType.REGULAR((7,)),
            pltpu.SemaphoreType.DMA((fields, 2)),
            pltpu.SemaphoreType.DMA((fields, 2)),
            pltpu.SemaphoreType.DMA((fields, 2)),
            pltpu.SemaphoreType.DMA((fields,)),
            pltpu.SemaphoreType.DMA((fields,)),
            pltpu.SemaphoreType.DMA((fields,)),
            pltpu.SemaphoreType.DMA((fields,)),
            pltpu.SemaphoreType.DMA((fields,)),
            pltpu.SemaphoreType.DMA((fields,)),
            pltpu.SemaphoreType.DMA((6,)),
        ],
        compiler_params=pltpu.CompilerParams(
            collective_id=0, has_side_effects=True, vmem_limit_bytes=20 * 2**20
        ),
    )(*(pltpu.with_memory_space_constraint(a, pltpu.HBM) for a in (field, *tables, symbol_x[None], symbol_y[None], symbol_z[None])))
    vmem = pl.BlockSpec(memory_space=pltpu.VMEM)
    return pl.pallas_call(
        finish,
        out_shape=jax.ShapeDtypeStruct((fields, share_x, share_k, grid_z), jnp.float32),
        in_specs=[vmem] * 4,
        out_specs=pl.BlockSpec(memory_space=pltpu.HBM),
        scratch_shapes=[
            pltpu.VMEM((share_x, share_k, grid_z), jnp.float32),
            pltpu.SemaphoreType.DMA((fields + 1,)),
        ],
        compiler_params=pltpu.CompilerParams(vmem_limit_bytes=8 * 2**20),
    )(done, landed, table_z, symbol)


def solution(mesh):
    rows, cols = mesh.shape["row"], mesh.shape["col"]

    def whole(species, symbol_x, symbol_y, symbol_z):
        _, grid_x, grid_y, grid_z = species.shape
        share_y = grid_y // rows
        order = np.arange(grid_y).reshape(rows, share_y).T.reshape(-1)
        tables = (
            jnp.asarray(halves_of(transform_table(grid_x))),
            jnp.asarray(halves_of(transform_table(grid_y)[:, order])),
            jnp.asarray(halves_of(transform_table(grid_z))),
        )
        return jax.shard_map(
            functools.partial(on_device, rows, cols),
            mesh=mesh,
            in_specs=((P(), P(), P()), P(None, None, "row", "col"), P(), P(), P()),
            out_specs=P(None, "row", "col", None),
            check_vma=False,
        )(tables, species, symbol_x, symbol_y, symbol_z)

    return whole
```
